32 devices in a mesh: col: 16 (over z, y, x), sec: 2 (over core).
Axes of the slice: x: 2, y: 2, z: 4, core: 2. Of those that a mesh axis runs over, the one named last changes fastest.
Arguments:
- mps: bfloat16 [16, 96, 6, 6, 96], P('col', 'sec'), may hold values from -6 to 6
- ket: bfloat16 [16, 6, 6, 6, 6, 2], P('col'), may hold values from -6 to 6
- left_proj: bfloat16 [16, 96, 96, 6, 6], P('col', 'sec'), may hold values from -0.109375 to 0.109375
- right_proj: bfloat16 [16, 96, 6, 6, 96], P('col', None, None, None, 'sec'), may hold values from -0.109375 to 0.109375
- bond_charge: int32 [16, 96], P('col'), may hold values from 0 to 5
- new_charge: int32 [16, 96], P('col'), may hold values from 0 to 5
- link_charge: int32 [16, 6], P('col'), may hold values from 0 to 2
- vert_charge: int32 [16, 2, 6], P('col'), may hold values from 0 to 2
Outputs:
- new_mps: bfloat16 [16, 96, 6, 6, 96], P('col', 'sec')
- log_norm: float32 [], replicated
The draws below stay inside these ranges and needn't reach their ends.
All inputs are finite; a program needn't handle non-finite values.
Results may differ from the reference program's by a relative error of at most 0.0064.
Values may be sent and summed in bfloat16 or wider, within the bound.
A program may use at most 192 MiB of HBM per device.

```python
import jax
import jax.numpy as jnp
from jax import lax

CHI = 96
D = 6
P_SIZE = 2
SITES = 16


def with_ends(values, key, least, top_value):
    dims = values.shape
    index_at = [jax.random.randint(jax.random.fold_in(key, axis), (), 0, dims[axis]) for axis in range(len(dims))]
    values = values.at[tuple(index_at)].set(least)
    longest = dims.index(max(dims))
    index_at[longest] = (index_at[longest] + 1) % dims[longest]
    return values.at[tuple(index_at)].set(top_value)


def steps_of(rng, extent, split, low, largest):
    loudness = 1.0
    for dim, blocks in split:
        draws = jax.random.uniform(jax.random.fold_in(jax.random.fold_in(rng, 6), dim), (blocks,), jnp.float32, low / len(split), largest / len(split))
        loudness = loudness * jnp.repeat(jnp.exp(draws), extent[dim] // blocks).reshape((-1,) + (1,) * (len(extent) - 1 - dim))
    return loudness


def normal_values(stream_key, extent, deviation, most, cuts=(), held_as=jnp.bfloat16):
    entries = jax.random.normal(stream_key, extent, jnp.float32) * deviation
    if len(cuts) > 0:
        entries = steps_of(stream_key, extent, cuts, -0.22, 0.18) * entries
    return jnp.clip(entries, min=-most, max=most).astype(held_as)


def setup_inputs(seed: int = 0) -> dict:
    key_of = jax.random.split(jax.random.key(seed), 9)
    return {
        "mps": normal_values(key_of[0], (SITES, CHI, D, D, CHI), 1.0, 6.0, ((0, 16), (1, 2))),
        "ket": normal_values(key_of[1], (SITES, D, D, D, D, P_SIZE), 1.0, 6.0, ((0, 16),)),
        "left_proj": normal_values(key_of[2], (SITES, CHI, CHI, D, D), (CHI * D * D) ** -0.5, 0.109375, ((0, 16), (1, 2))),
        "right_proj": normal_values(key_of[3], (SITES, CHI, D, D, CHI), (CHI * D * D) ** -0.5, 0.109375, ((0, 16), (4, 2))),
        "bond_charge": with_ends(jax.random.randint(key_of[4], (SITES, CHI), 0, 6), jax.random.fold_in(key_of[4], 1), 0, 5).astype(jnp.int32),
        "new_charge": with_ends(jax.random.randint(key_of[5], (SITES, CHI), 0, 6), jax.random.fold_in(key_of[5], 1), 0, 5).astype(jnp.int32),
        "link_charge": with_ends(jax.random.randint(key_of[6], (SITES, D), 0, 3), jax.random.fold_in(key_of[6], 1), 0, 2).astype(jnp.int32),
        "vert_charge": with_ends(jax.random.randint(key_of[7], (SITES, 2, D), 0, 3), jax.random.fold_in(key_of[7], 1), 0, 2).astype(jnp.int32),
    }


def absorb(mps_site, ket_site, left_site, right_site, charge_here, charge_next, fresh_here, fresh_next, link_here, link_next, vertical):
    upper = vertical[0]
    lower = vertical[1]
    physical = jnp.arange(ket_site.shape[4], dtype=jnp.int32)
    keep_mps = charge_here[:, None, None, None] + upper[None, :, None, None] - upper[None, None, :, None] == charge_next[None, None, None, :]
    masked_mps = jnp.where(keep_mps, mps_site, jnp.zeros_like(mps_site))
    keep_ket = upper[:, None, None, None, None] + link_here[None, :, None, None, None] == lower[None, None, :, None, None] + link_next[None, None, None, :, None] + physical[None, None, None, None, :]
    masked_ket = jnp.where(keep_ket, ket_site, jnp.zeros_like(ket_site))
    keep_left = fresh_here[:, None, None, None] == charge_here[None, :, None, None] + link_here[None, None, :, None] - link_here[None, None, None, :]
    masked_left = jnp.where(keep_left, left_site, jnp.zeros_like(left_site))
    keep_right = charge_next[:, None, None, None] + link_next[None, :, None, None] - link_next[None, None, :, None] == fresh_next[None, None, None, :]
    masked_right = jnp.where(keep_right, right_site, jnp.zeros_like(right_site))
    ket_wide = masked_ket.astype(jnp.float32)
    first = jnp.einsum('xalm,auvb->xlmuvb', masked_left.astype(jnp.float32), masked_mps.astype(jnp.float32)).astype(jnp.bfloat16)
    second = jnp.einsum('xlmuvb,uldrp->xmvbdrp', first.astype(jnp.float32), ket_wide).astype(jnp.bfloat16)
    third = jnp.einsum('xmvbdrp,vmesp->xbdres', second.astype(jnp.float32), ket_wide).astype(jnp.bfloat16)
    return jnp.einsum('xbdres,brsy->xdey', third.astype(jnp.float32), masked_right.astype(jnp.float32))

def reference(mps, ket, left_proj, right_proj, bond_charge, new_charge, link_charge, vert_charge):

    def following(array):
        return jnp.roll(array, -1, axis=0)
    items = (mps, ket, left_proj, following(right_proj), bond_charge, following(bond_charge), new_charge, following(new_charge), link_charge, following(link_charge), vert_charge)

    def single(item):
        return absorb(*item)
    image = lax.map(single, items)
    count = CHI * D * D * CHI
    meansq = lax.optimization_barrier(jnp.sum(image * image, axis=(1, 2, 3, 4))) / count
    scale = lax.rsqrt(meansq + 1e-06)
    new_mps = (image * scale[:, None, None, None, None]).astype(jnp.bfloat16)
    log_norm = jnp.mean(0.5 * jnp.log(meansq + 1e-06))
    return (new_mps, log_norm)
```

```python
import functools
import math

import jax
import jax.numpy as jnp
from jax import lax
from jax.experimental import pallas as pl
from jax.experimental.pallas import tpu as pltpu
from jax.sharding import PartitionSpec as P

LANES = 128
F32 = jnp.float32
BF16 = jnp.bfloat16
MESH = pl.DeviceIdType.MESH


def layout(chi, half, legs):
    span = math.lcm(chi, LANES)
    group, tiles = span // chi, span // LANES
    pieces = []
    for t in range(tiles):
        row = []
        for g in range(group):
            lo, hi = max(LANES * t, chi * g), min(LANES * (t + 1), chi * (g + 1))
            if lo < hi:
                row.append((g, lo - LANES * t, hi - LANES * t))
        pieces.append(row)
    assert all(len(row) == 2 and row[1][0] == row[0][0] + 1 for row in pieces)
    assert half % (2 * group) == 0 and half % 16 == 0 and chi <= LANES and legs % 2 == 0
    pad = -(-legs * legs // 8) * 8
    return group, tiles, half // group, pad, pieces


def chain(
    legs, phys, count, cols, secs,
    left_hbm, mps_hbm, right_hbm, ket_ref, bond_ref, fresh_ref, link_ref, link_sm, vert_sm,
    out_ref, log_ref,
    left_v, mps_all, right_all, left_s, left_b, rhs1, rhs4, raw_s, whole_s, w1, w2, w3, image_s, clean_s,
    charge_here, charge_next, diff, rowkey, lanekey,
    stage, slots, local_sem, near_send, near_recv, send_sem, recv_sem,
):
    total = cols * secs
    square = legs * legs
    half, chi = left_v.shape[1:]
    group, tiles, quads, pad, pieces = layout(chi, half, legs)
    deep = legs * pad
    block = quads * pad
    pairs = legs // 2
    me_col, me_sec = lax.axis_index("col"), lax.axis_index("sec")
    me = me_col * secs + me_sec
    before = lax.rem(me_col + cols - 1, cols)
    barrier = pltpu.get_barrier_semaphore()
    mine = pl.ds(pl.multiple_of(me_sec * half, 16), half)

    def other(k):
        at = lax.rem(me + k, total)
        return at, (at // secs, lax.rem(at, secs))

    def close(k):
        at = me_col * secs + lax.rem(me_sec + k, secs)
        return lax.rem(at - me + total, total)

    def charge_copy():
        return pltpu.make_async_remote_copy(
            src_ref=charge_here, dst_ref=charge_next, send_sem=near_send.at[0], recv_sem=near_recv.at[0],
            device_id=(before, me_sec), device_id_type=MESH,
        )

    def mps_copy(k, source):
        return pltpu.make_async_remote_copy(
            src_ref=mps_hbm, dst_ref=mps_all.at[source], send_sem=near_send.at[k],
            recv_sem=near_recv.at[1 + source],
            device_id=(me_col, lax.rem(me_sec + k, secs)), device_id_type=MESH,
        )

    def right_copy():
        return pltpu.make_async_remote_copy(
            src_ref=right_hbm, dst_ref=right_all.at[me_sec], send_sem=near_send.at[secs],
            recv_sem=near_recv.at[1 + secs + me_sec],
            device_id=(before, me_sec), device_id_type=MESH,
        )

    def right_pass(k, source):
        return pltpu.make_async_remote_copy(
            src_ref=right_all.at[source], dst_ref=right_all.at[source], send_sem=near_send.at[secs + k],
            recv_sem=near_recv.at[1 + secs + source],
            device_id=(me_col, lax.rem(me_sec + k, secs)), device_id_type=MESH,
        )

    def down_rows(row):
        return jnp.broadcast_to(row, (LANES, LANES)).T

    def over(value, by):
        return jnp.floor((value + 0.5) * (1.0 / by))

    def axis(shape, dim):
        return lax.broadcasted_iota(jnp.int32, shape, dim).astype(F32)

    def chosen(index, values):
        return sum(jnp.where(index == float(i), v, 0.0) for i, v in enumerate(values))

    load_left = pltpu.make_async_copy(left_hbm, left_v, local_sem.at[0])
    load_mps = pltpu.make_async_copy(mps_hbm, mps_all.at[me_sec], local_sem.at[1])
    load_left.start()
    load_mps.start()

    def greet(k, _):
        pl.semaphore_signal(barrier, inc=1, device_id=other(k)[1], device_id_type=MESH)
        return 0

    lax.fori_loop(1, total, greet, 0)
    charge_here[...] = jnp.zeros_like(charge_here)
    charge_here[0:1, 0:chi] = bond_ref[...]
    charge_here[1:2, 0:chi] = fresh_ref[...]
    charge_here[2:3, 0:legs] = link_ref[...]
    here = charge_here[...].astype(F32)
    diff[...] = down_rows(here[1:2]) - here[0:1]
    gaps_here = diff[mine, 0:chi]
    fresh_rows = down_rows(here[1:2])
    left_s[...] = jnp.zeros_like(left_s)
    for t in range(tiles):
        for k in range(2):
            rhs1[t, k * LANES + chi : (k + 1) * LANES] = jnp.zeros((LANES - chi, square * LANES), BF16)
            rhs4[t, k * LANES + chi : (k + 1) * LANES] = jnp.zeros((LANES - chi, square * LANES), BF16)

    small = (pad, 2 * LANES)
    row_in = axis(small, 0)
    row_mid = over(row_in, legs)
    row_last = row_in - legs * row_mid
    col = axis(small, 1)
    col_top = over(col, pad)
    col_in = col - pad * col_top
    col_mid = over(col_in, legs)
    col_last = col_in - legs * col_mid
    keys = square * legs * phys
    line = axis((pad, keys), 1)
    line_p = over(line, phys)
    line_d = line_p - legs * over(line_p, legs)
    line_p = line - phys * line_p
    tall = (keys, 2 * LANES)
    tall_in = over(axis(tall, 0), legs * phys)
    tall_u = over(tall_in, legs)
    tall_l = tall_in - legs * tall_u
    tall_col = axis(tall, 1)
    tall_top = over(tall_col, pad)
    tall_mid = over(tall_col - pad * tall_top, legs)
    spread_c = jnp.where(jnp.logical_and(tall_u == tall_top, tall_l == tall_mid), 1.0, 0.0).astype(BF16)
    ket = ket_ref[...]
    for r in range(legs):
        lead = jnp.where(axis((pad, legs), 1) == float(r), 1.0, 0.0).astype(BF16)
        grown = lax.dot_general(lead, ket, (((1,), (1,)), ((), ())), preferred_element_type=F32)
        for p in range(phys):
            keep = jnp.logical_and(line_d == row_last[:, 0:1], line_p == float(p))
            picked = jnp.where(keep, grown, 0.0).astype(BF16)
            raw_s[p, r * pad : (r + 1) * pad, :] = jnp.dot(picked, spread_c, preferred_element_type=F32)

    load_left.wait()
    for l in range(legs):
        for m in range(legs):
            gap = (link_sm[0, l] - link_sm[0, m]).astype(F32)
            value = jnp.where(gaps_here == gap, left_v[l * legs + m].astype(F32), 0.0)
            left_s[pl.ds(l * legs + m, half, stride=pad), 0:chi] = value
    left_b[...] = left_s[...].astype(BF16)

    pl.semaphore_wait(barrier, total - 1)
    charge_copy().start()
    for k in range(1, secs):
        mps_copy(k, me_sec).start()
    right_copy().start()

    lane = lax.broadcasted_iota(jnp.int32, (1, LANES), 1)

    def inside(lo, hi):
        return jnp.logical_and(lane >= lo, lane < hi)

    def turned(value):
        rest = jnp.zeros(value.shape[:-1] + (LANES - chi,), value.dtype)
        wide = jnp.concatenate([value, rest], axis=1)
        return [wide if (chi * g) % LANES == 0 else pltpu.roll(wide, (chi * g) % LANES, 1) for g in range(group)]

    def spread(value, dest, at, column):
        rolled = turned(value)
        for t in range(tiles):
            for k, (g, lo, hi) in enumerate(pieces[t]):
                piece = jnp.where(inside(lo, hi), rolled[g], 0.0)
                dest[t, k * LANES + at : k * LANES + at + half, column * LANES : (column + 1) * LANES] = piece.astype(BF16)

    load_mps.wait()
    for k in range(1, secs):
        mps_copy(k, lax.rem(me_sec + k, secs)).wait_recv()
    for k in range(secs):
        for u in range(legs):
            for v in range(legs):
                spread(mps_all[k, u * legs + v].astype(F32), rhs1, k * half, v * legs + u)

    for t in range(tiles):
        lhs = jnp.concatenate([left_b[g * block : (g + 1) * block] for g, _, _ in pieces[t]], axis=1)

        def first(i, _, t=t, lhs=lhs):
            part = jnp.dot(lhs, rhs1[t, :, pl.ds(pl.multiple_of(i * 2 * LANES, 2 * LANES), 2 * LANES)], preferred_element_type=F32)
            for q in range(quads):
                rows = part[q * pad : (q + 1) * pad]
                both = jnp.concatenate([rows[:, :LANES], rows[:, LANES:]], axis=0).astype(BF16)
                at = pl.ds(pl.multiple_of((i % pairs) * 2 * pad, 16), 2 * pad)
                w1[t, q // 2, i // pairs, at, (q % 2) * LANES : (q % 2 + 1) * LANES] = both
            return 0

        lax.fori_loop(0, pairs * legs, first, 0, unroll=True)

    charge_copy().wait_recv()
    after = charge_next[...].astype(F32)

    col_key = chosen(col_top, [vert_sm[0, i].astype(F32) for i in range(legs)])
    col_key += chosen(col_mid, [link_sm[0, i].astype(F32) for i in range(legs)])
    row_key = chosen(row_last, [vert_sm[1, i].astype(F32) for i in range(legs)])
    same = jnp.logical_and(row_mid == col_last, jnp.logical_and(row_in < square, col_in < square))
    for r in range(legs):
        lack = col_key - row_key - after[2:3, r : r + 1]
        value = jnp.zeros(small, F32)
        for p in range(phys):
            value += jnp.where(lack == float(p), raw_s[p, r * pad : (r + 1) * pad, :], 0.0)
        whole_s[r * pad : (r + 1) * pad, :] = jnp.where(same, value, 0.0)
    both_rows = whole_s[:, 0:deep].astype(BF16)

    ups = [vert_sm[0, i].astype(F32) for i in range(legs)]
    mid_key = chosen(row_last, [link_sm[0, i].astype(F32) for i in range(legs)])
    mid_key -= chosen(row_mid, [link_sm[0, i].astype(F32) for i in range(legs)])
    for v in range(legs):
        for u in range(pairs):
            pair = jnp.concatenate([mid_key[:, :LANES] + (ups[2 * u + k] - ups[v]) for k in range(2)], axis=0)
            rowkey[v, u * 2 * pad : (u + 1) * 2 * pad] = pair.astype(BF16)
    turned_next = turned(after[0:1, 0:chi])
    diff[...] = fresh_rows
    for t in range(tiles):
        for q in range(quads):
            key = jnp.zeros((16, LANES), F32)
            for g, lo, hi in pieces[t]:
                own = diff[pl.ds(me_sec * half + g * quads + q, 1), :]
                key += jnp.where(inside(lo, hi), turned_next[g] - own, 0.0)
            lanekey[t, q // 2, :, (q % 2) * LANES : (q % 2 + 1) * LANES] = key.astype(BF16)

    def second(n, slot):
        t, j = n // (quads // 2), n % (quads // 2)
        key = lanekey[t, j][None]
        for vp in range(pairs):
            parts = []
            for k in range(2):
                rows = rowkey[2 * vp + k]
                rows = jnp.concatenate([rows, rows], axis=1).reshape(deep // 16, 16, 2 * LANES)
                value = w1[t, j, 2 * vp + k].reshape(deep // 16, 16, 2 * LANES)
                value = jnp.where(rows == key, value, jnp.zeros_like(value)).reshape(deep, 2 * LANES)
                parts.append(jnp.dot(both_rows, value, preferred_element_type=F32))
            for r in range(legs):
                both = jnp.concatenate([part[r * pad : (r + 1) * pad] for part in parts], axis=0)
                w2[slot, r, vp * 2 * pad : (vp + 1) * 2 * pad, :] = both.astype(BF16)

    def third(n, slot):
        t, j = n // (quads // 2), n % (quads // 2)
        at = pl.ds(pl.multiple_of(j * 2 * pad, 16), 2 * pad)
        for r in range(legs):
            part = jnp.dot(both_rows, w2[slot, r], preferred_element_type=F32)
            for s in range(legs):
                rows = part[s * pad : (s + 1) * pad]
                both = jnp.concatenate([rows[:, :LANES], rows[:, LANES:]], axis=0).astype(BF16)
                w3[t, at, (r * legs + s) * LANES : (r * legs + s + 1) * LANES] = both

    steps = tiles * (quads // 2)

    def middle(n, _):
        second(n, n % 2)
        third(n - 1, (n + 1) % 2)
        return 0

    second(0, 0)
    lax.fori_loop(1, steps // 2, middle, 0, unroll=True)
    right_copy().wait_recv()
    for k in range(1, secs):
        right_pass(k, me_sec).start()
    lax.fori_loop(steps // 2, steps, middle, 0, unroll=True)
    third(steps - 1, (steps - 1) % 2)

    diff[...] = down_rows(after[1:2]) - after[0:1]
    for k in range(1, secs):
        right_pass(k, lax.rem(me_sec + k, secs)).wait_recv()
    for k in range(secs):
        delta = diff[k * half : (k + 1) * half, 0:chi]
        for r in range(legs):
            for s in range(legs):
                gap = after[2:3, r : r + 1] - after[2:3, s : s + 1]
                value = jnp.where(delta == gap, right_all[k, r * legs + s].astype(F32), 0.0)
                spread(value, rhs4, k * half, r * legs + s)

    seen = set()
    for t in range(tiles):
        part = lax.dot_general(w3[t], rhs4[t], (((1,), (1,)), ((), ())), preferred_element_type=F32)
        for k, (g, _, _) in enumerate(pieces[t]):
            value = part[:, k * LANES : (k + 1) * LANES]
            if g in seen:
                value += image_s[g * block : (g + 1) * block]
            seen.add(g)
            image_s[g * block : (g + 1) * block] = value

    diff[...] = fresh_rows + after[1:2]
    odd = diff[mine, 0:chi]
    odd = odd - 2.0 * jnp.floor(odd * 0.5)
    total_sq = jnp.zeros((half, chi), F32)
    for d in range(legs):
        for e in range(legs):
            value = image_s[pl.ds(d * legs + e, half, stride=pad), 0:chi]
            parity = ((vert_sm[1, d] + vert_sm[1, e]) & 1).astype(F32)
            value = jnp.where(odd == parity, value, 0.0)
            clean_s[d * legs + e] = value
            total_sq += value * value
    part = jnp.sum(jnp.sum(total_sq, axis=0, keepdims=True), axis=1, keepdims=True)
    stage[...] = jnp.broadcast_to(part, stage.shape)
    slots[me] = jnp.broadcast_to(part, stage.shape)

    def copy_to(k):
        at, where = other(k)
        return pltpu.make_async_remote_copy(
            src_ref=stage, dst_ref=slots.at[me], send_sem=send_sem.at[k], recv_sem=recv_sem.at[me],
            device_id=where, device_id_type=MESH,
        )

    def send(k, _):
        copy_to(k).start()
        return 0

    def receive(k, _):
        at, where = other(k)
        pltpu.make_async_remote_copy(
            src_ref=stage, dst_ref=slots.at[at], send_sem=send_sem.at[k], recv_sem=recv_sem.at[at],
            device_id=where, device_id_type=MESH,
        ).wait_recv()
        return 0

    def sent(k, _):
        copy_to(k).wait_send()
        return 0

    lax.fori_loop(1, total, send, 0)
    site = jnp.broadcast_to(part, stage.shape)
    for k in range(1, secs):
        receive(close(k), 0)
        site = site + slots[me_col * secs + lax.rem(me_sec + k, secs)]
    scale = lax.rsqrt(site[0:1, 0:1] / count + 1e-06)
    for i in range(square):
        out_ref[i] = (clean_s[i] * scale).astype(BF16)

    def receive_far(k, _):
        at, _where = other(k)

        @pl.when(at // secs != me_col)
        def _():
            receive(k, 0)

        return 0

    lax.fori_loop(1, total, receive_far, 0)
    sums = jnp.sum(slots[...].reshape(cols, secs, 1, LANES), axis=1) / count
    logs = jnp.sum(0.5 * jnp.log(sums + 1e-06), axis=0) / cols
    log_ref[...] = logs[0:1, 0:1]
    lax.fori_loop(1, total, sent, 0)
    charge_copy().wait_send()
    for k in range(1, secs):
        mps_copy(k, me_sec).wait_send()
    right_copy().wait_send()
    for k in range(1, secs):
        right_pass(k, me_sec).wait_send()


def local(mps, ket, left_proj, right_proj, bond_charge, new_charge, link_charge, vert_charge):
    half, chi, legs = left_proj.shape[1:4]
    phys = ket.shape[5]
    assert phys == 2
    square = legs * legs
    cols, secs = lax.axis_size("col"), lax.axis_size("sec")
    group, tiles, quads, pad, pieces = layout(chi, half, legs)
    deep, block = legs * pad, quads * pad
    assert deep <= 2 * LANES
    arrays = [
        left_proj[0].transpose(2, 3, 0, 1).reshape(square, half, chi),
        mps[0].transpose(1, 2, 0, 3).reshape(square, half, chi),
        right_proj[0].transpose(1, 2, 3, 0).reshape(square, half, chi),
        ket[0].transpose(0, 1, 2, 4, 3).reshape(square * legs * phys, legs),
        bond_charge,
        new_charge,
        link_charge,
        link_charge,
        vert_charge[0],
    ]
    far = pl.BlockSpec(memory_space=pl.ANY)
    near = pl.BlockSpec(memory_space=pltpu.VMEM)
    scalar = pl.BlockSpec(memory_space=pltpu.SMEM)
    image, logs = pl.pallas_call(
        functools.partial(chain, legs, phys, chi * square * chi, cols, secs),
        in_specs=[far] * 3 + [near] * 4 + [scalar] * 2,
        out_specs=[near, near],
        out_shape=[jax.ShapeDtypeStruct((square, half, chi), BF16), jax.ShapeDtypeStruct((1, 1), F32)],
        scratch_shapes=[
            pltpu.VMEM((square, half, chi), BF16),
            pltpu.VMEM((secs, square, half, chi), BF16),
            pltpu.VMEM((secs, square, half, chi), BF16),
            pltpu.VMEM((half * pad, LANES), F32),
            pltpu.VMEM((half * pad, LANES), BF16),
            pltpu.VMEM((tiles, 2 * LANES, square * LANES), BF16),
            pltpu.VMEM((tiles, 2 * LANES, square * LANES), BF16),
            pltpu.VMEM((phys, deep, 2 * LANES), F32),
            pltpu.VMEM((deep, 2 * LANES), F32),
            pltpu.VMEM((tiles, quads // 2, legs, deep, 2 * LANES), BF16),
            pltpu.VMEM((2, legs, deep, 2 * LANES), BF16),
            pltpu.VMEM((tiles, block, square * LANES), BF16),
            pltpu.VMEM((half * pad, LANES), F32),
            pltpu.VMEM((square, half, chi), F32),
            pltpu.VMEM((8, LANES), jnp.int32),
            pltpu.VMEM((8, LANES), jnp.int32),
            pltpu.VMEM((LANES, LANES), F32),
            pltpu.VMEM((legs, deep, LANES), BF16),
            pltpu.VMEM((tiles, quads // 2, 16, 2 * LANES), BF16),
            pltpu.VMEM((1, LANES), F32),
            pltpu.VMEM((cols * secs, 1, LANES), F32),
            pltpu.SemaphoreType.DMA((2,)),
            pltpu.SemaphoreType.DMA((2 * secs,)),
            pltpu.SemaphoreType.DMA((1 + 2 * secs,)),
            pltpu.SemaphoreType.DMA((cols * secs,)),
            pltpu.SemaphoreType.DMA((cols * secs,)),
        ],
        compiler_params=pltpu.CompilerParams(
            vmem_limit_bytes=62 * 1024 * 1024,
            collective_id=0,
            has_side_effects=True,
        ),
    )(*arrays)
    new_mps = image.reshape(legs, legs, half, chi).transpose(2, 0, 1, 3)[None]
    return (new_mps, logs[0, 0])


def solution(mesh):
    placed = (
        P("col", "sec", None, None, None),
        P("col", None, None, None, None, None),
        P("col", "sec", None, None, None),
        P("col", None, None, None, "sec"),
        P("col", None),
        P("col", None),
        P("col", None),
        P("col", None, None),
    )
    return jax.shard_map(
        local,
        mesh=mesh,
        in_specs=placed,
        out_specs=(P("col", "sec", None, None, None), P()),
        check_vma=False,
    )
```

```python
import functools
import math

import jax
import jax.numpy as jnp
from jax import lax
from jax.experimental import pallas as pl
from jax.experimental.pallas import tpu as pltpu
from jax.sharding import PartitionSpec as P

LANES = 128
F32 = jnp.float32
BF16 = jnp.bfloat16
MESH = pl.DeviceIdType.MESH


def layout(chi, half, legs):
    span = math.lcm(chi, LANES)
    group, tiles = span // chi, span // LANES
    pieces = []
    for t in range(tiles):
        row = []
        for g in range(group):
            lo, hi = max(LANES * t, chi * g), min(LANES * (t + 1), chi * (g + 1))
            if lo < hi:
                row.append((g, lo - LANES * t, hi - LANES * t))
        pieces.append(row)
    assert all(len(row) == 2 and row[1][0] == row[0][0] + 1 for row in pieces)
    assert half % (2 * group) == 0 and half % 16 == 0 and chi <= LANES and legs % 2 == 0
    pad = -(-legs * legs // 8) * 8
    return group, tiles, half // group, pad, pieces


def chain(
    legs, phys, count, cols, secs,
    left_hbm, mps_hbm, right_hbm, ket_ref, bond_ref, fresh_ref, link_ref, link_sm, vert_sm,
    out_ref, log_ref,
    left_v, mps_all, right_all, left_s, left_b, rhs1, rhs4, raw_s, whole_s, w1, w2, w3, image_s, clean_s,
    charge_here, charge_next, diff, rowkey, lanekey,
    stage, slots, close_slots, local_sem, near_send, near_recv, chunk_send, chunk_recv, pass_send, pass_recv,
    known, far_send, far_recv, close_send, close_recv,
):
    square = legs * legs
    half, chi = left_v.shape[1:]
    group, tiles, quads, pad, pieces = layout(chi, half, legs)
    deep = legs * pad
    block = quads * pad
    pairs = legs // 2
    me_col, me_sec = lax.axis_index("col"), lax.axis_index("sec")
    before = lax.rem(me_col + cols - 1, cols)
    barrier = pltpu.get_barrier_semaphore()
    mine = pl.ds(pl.multiple_of(me_sec * half, 16), half)

    chunks = right_all.shape[1]
    own = right_all.shape[2]

    def column(k):
        return lax.rem(me_col + k + cols, cols)

    def partner(k):
        return (me_col, lax.rem(me_sec + k, secs))

    def charge_copy():
        return pltpu.make_async_remote_copy(
            src_ref=charge_here, dst_ref=charge_next, send_sem=near_send.at[0], recv_sem=near_recv.at[0],
            device_id=(before, me_sec), device_id_type=MESH,
        )

    def mps_copy(k, source):
        return pltpu.make_async_remote_copy(
            src_ref=mps_hbm, dst_ref=mps_all.at[source], send_sem=near_send.at[k],
            recv_sem=near_recv.at[1 + source],
            device_id=partner(k), device_id_type=MESH,
        )

    def right_copy(c):
        return pltpu.make_async_remote_copy(
            src_ref=right_hbm.at[pl.ds(c * own, own)], dst_ref=right_all.at[me_sec, c],
            send_sem=chunk_send.at[c], recv_sem=chunk_recv.at[c],
            device_id=(before, me_sec), device_id_type=MESH,
        )

    def right_pass(c, k, source):
        return pltpu.make_async_remote_copy(
            src_ref=right_all.at[source, c], dst_ref=right_all.at[source, c],
            send_sem=pass_send.at[c, k], recv_sem=pass_recv.at[c, source],
            device_id=partner(k), device_id_type=MESH,
        )

    def arrived(c):
        right_copy(c).wait_recv()
        for k in range(1, secs):
            right_pass(c, k, me_sec).start()

    def passed(c):
        for k in range(1, secs):
            right_pass(c, k, lax.rem(me_sec + k, secs)).wait_recv()

    rounds = max(1, (cols // 2 - 1).bit_length())

    def tell(n):
        if n < rounds:
            for side in (-1, 1):
                pl.semaphore_signal(
                    known.at[n], inc=1, device_id=(column(side * 2**n), me_sec), device_id_type=MESH
                )

    def hear(n):
        if n < rounds:
            pl.semaphore_wait(known.at[n], 2)

    def down_rows(row):
        return jnp.broadcast_to(row, (LANES, LANES)).T

    def over(value, by):
        return jnp.floor((value + 0.5) * (1.0 / by))

    def axis(shape, dim):
        return lax.broadcasted_iota(jnp.int32, shape, dim).astype(F32)

    def chosen(index, values):
        return sum(jnp.where(index == float(i), v, 0.0) for i, v in enumerate(values))

    load_left = pltpu.make_async_copy(left_hbm, left_v, local_sem.at[0])
    load_mps = pltpu.make_async_copy(mps_hbm, mps_all.at[me_sec], local_sem.at[1])
    load_left.start()
    load_mps.start()

    for k in range(1, secs):
        pl.semaphore_signal(barrier, inc=1, device_id=partner(k), device_id_type=MESH)
    for side in (-1, 1):
        pl.semaphore_signal(barrier, inc=1, device_id=(column(side), me_sec), device_id_type=MESH)
    charge_here[...] = jnp.zeros_like(charge_here)
    charge_here[0:1, 0:chi] = bond_ref[...]
    charge_here[1:2, 0:chi] = fresh_ref[...]
    charge_here[2:3, 0:legs] = link_ref[...]
    here = charge_here[...].astype(F32)
    diff[...] = down_rows(here[1:2]) - here[0:1]
    gaps_here = diff[mine, 0:chi]
    fresh_rows = down_rows(here[1:2])
    left_s[...] = jnp.zeros_like(left_s)
    for t in range(tiles):
        for k in range(2):
            rhs1[t, k * LANES + chi : (k + 1) * LANES] = jnp.zeros((LANES - chi, square * LANES), BF16)
            for c in range(chunks):
                rhs4[c][t, k * LANES + chi : (k + 1) * LANES] = jnp.zeros((LANES - chi, own * LANES), BF16)

    lane = lax.broadcasted_iota(jnp.int32, (1, LANES), 1)

    def inside(lo, hi):
        return jnp.logical_and(lane >= lo, lane < hi)

    def turned(value):
        rest = jnp.zeros(value.shape[:-1] + (LANES - chi,), value.dtype)
        wide = jnp.concatenate([value, rest], axis=1)
        return [wide if (chi * g) % LANES == 0 else pltpu.roll(wide, (chi * g) % LANES, 1) for g in range(group)]

    def spread(value, dest, at, place):
        rolled = turned(value)
        for t in range(tiles):
            for k, (g, lo, hi) in enumerate(pieces[t]):
                piece = jnp.where(inside(lo, hi), rolled[g], 0.0)
                dest[t, pl.ds(k * LANES + at, half), place * LANES : (place + 1) * LANES] = piece.astype(BF16)

    load_left.wait()
    for l in range(legs):
        for m in range(legs):
            gap = (link_sm[0, l] - link_sm[0, m]).astype(F32)
            value = jnp.where(gaps_here == gap, left_v[l * legs + m].astype(F32), 0.0)
            left_s[pl.ds(l * legs + m, half, stride=pad), 0:chi] = value
    left_b[...] = left_s[...].astype(BF16)

    def half_one(source):
        at = pl.multiple_of(source * half, 16)
        for u in range(legs):
            for v in range(legs):
                spread(mps_all[source, u * legs + v].astype(F32), rhs1, at, v * legs + u)

    load_mps.wait()
    half_one(me_sec)

    pl.semaphore_wait(barrier, secs + 1)
    charge_copy().start()
    for k in range(1, secs):
        mps_copy(k, me_sec).start()
    for c in range(chunks):
        right_copy(c).start()
    tell(0)

    small = (pad, 2 * LANES)
    row_in = axis(small, 0)
    row_mid = over(row_in, legs)
    row_last = row_in - legs * row_mid
    col = axis(small, 1)
    col_top = over(col, pad)
    col_in = col - pad * col_top
    col_mid = over(col_in, legs)
    col_last = col_in - legs * col_mid
    keys = square * legs * phys
    line = axis((pad, keys), 1)
    line_p = over(line, phys)
    line_d = line_p - legs * over(line_p, legs)
    line_p = line - phys * line_p
    tall = (keys, 2 * LANES)
    tall_in = over(axis(tall, 0), legs * phys)
    tall_u = over(tall_in, legs)
    tall_l = tall_in - legs * tall_u
    tall_col = axis(tall, 1)
    tall_top = over(tall_col, pad)
    tall_mid = over(tall_col - pad * tall_top, legs)
    spread_c = jnp.where(jnp.logical_and(tall_u == tall_top, tall_l == tall_mid), 1.0, 0.0).astype(BF16)
    lead = jnp.where(over(axis((deep, legs), 0), pad) == axis((deep, legs), 1), 1.0, 0.0).astype(BF16)
    grown = lax.dot_general(lead, ket_ref[...], (((1,), (1,)), ((), ())), preferred_element_type=F32)
    same_d = line_d == row_last[:, 0:1]
    for p in range(phys):
        keep = jnp.logical_and(same_d, line_p == float(p))
        picked = [jnp.where(keep, grown[r * pad : (r + 1) * pad], 0.0) for r in range(legs)]
        picked = jnp.concatenate(picked, axis=0).astype(BF16)
        raw_s[p] = jnp.dot(picked, spread_c, preferred_element_type=F32)

    for k in range(1, secs):
        source = lax.rem(me_sec + k, secs)
        mps_copy(k, source).wait_recv()
        half_one(source)

    for t in range(tiles):
        lhs = jnp.concatenate([left_b[g * block : (g + 1) * block] for g, _, _ in pieces[t]], axis=1)

        def first(i, _, t=t, lhs=lhs):
            part = jnp.dot(lhs, rhs1[t, :, pl.ds(pl.multiple_of(i * 2 * LANES, 2 * LANES), 2 * LANES)], preferred_element_type=F32)
            for q in range(quads):
                rows = part[q * pad : (q + 1) * pad]
                both = jnp.concatenate([rows[:, :LANES], rows[:, LANES:]], axis=0).astype(BF16)
                at = pl.ds(pl.multiple_of((i % pairs) * 2 * pad, 16), 2 * pad)
                w1[t, q // 2, i // pairs, at, (q % 2) * LANES : (q % 2 + 1) * LANES] = both
            return 0

        lax.fori_loop(0, pairs * legs, first, 0, unroll=True)

    hear(0)
    tell(1)
    charge_copy().wait_recv()
    after = charge_next[...].astype(F32)

    col_key = chosen(col_top, [vert_sm[0, i].astype(F32) for i in range(legs)])
    col_key += chosen(col_mid, [link_sm[0, i].astype(F32) for i in range(legs)])
    row_key = chosen(row_last, [vert_sm[1, i].astype(F32) for i in range(legs)])
    same = jnp.logical_and(row_mid == col_last, jnp.logical_and(row_in < square, col_in < square))
    for r in range(legs):
        lack = col_key - row_key - after[2:3, r : r + 1]
        value = jnp.zeros(small, F32)
        for p in range(phys):
            value += jnp.where(lack == float(p), raw_s[p, r * pad : (r + 1) * pad, :], 0.0)
        whole_s[r * pad : (r + 1) * pad, :] = jnp.where(same, value, 0.0)
    both_rows = whole_s[:, 0:deep].astype(BF16)

    ups = [vert_sm[0, i].astype(F32) for i in range(legs)]
    mid_key = chosen(row_last, [link_sm[0, i].astype(F32) for i in range(legs)])
    mid_key -= chosen(row_mid, [link_sm[0, i].astype(F32) for i in range(legs)])
    for v in range(legs):
        for u in range(pairs):
            pair = jnp.concatenate([mid_key[:, :LANES] + (ups[2 * u + k] - ups[v]) for k in range(2)], axis=0)
            rowkey[v, u * 2 * pad : (u + 1) * 2 * pad] = pair.astype(BF16)
    turned_next = turned(after[0:1, 0:chi])
    diff[...] = fresh_rows
    for t in range(tiles):
        for q in range(quads):
            key = jnp.zeros((16, LANES), F32)
            for g, lo, hi in pieces[t]:
                fresh = diff[pl.ds(me_sec * half + g * quads + q, 1), :]
                key += jnp.where(inside(lo, hi), turned_next[g] - fresh, 0.0)
            lanekey[t, q // 2, :, (q % 2) * LANES : (q % 2 + 1) * LANES] = key.astype(BF16)

    def second(n, slot):
        t, j = n // (quads // 2), n % (quads // 2)
        key = lanekey[t, j][None]
        for vp in range(pairs):
            parts = []
            for k in range(2):
                rows = rowkey[2 * vp + k]
                rows = jnp.concatenate([rows, rows], axis=1).reshape(deep // 16, 16, 2 * LANES)
                value = w1[t, j, 2 * vp + k].reshape(deep // 16, 16, 2 * LANES)
                value = jnp.where(rows == key, value, jnp.zeros_like(value)).reshape(deep, 2 * LANES)
                parts.append(jnp.dot(both_rows, value, preferred_element_type=F32))
            for r in range(legs):
                both = jnp.concatenate([part[r * pad : (r + 1) * pad] for part in parts], axis=0)
                w2[slot, r, vp * 2 * pad : (vp + 1) * 2 * pad, :] = both.astype(BF16)

    def third(n, slot):
        t, j = n // (quads // 2), n % (quads // 2)
        at = pl.ds(pl.multiple_of(j * 2 * pad, 16), 2 * pad)
        for r in range(legs):
            part = jnp.dot(both_rows, w2[slot, r], preferred_element_type=F32)
            for s in range(legs):
                rows = part[s * pad : (s + 1) * pad]
                both = jnp.concatenate([rows[:, :LANES], rows[:, LANES:]], axis=0).astype(BF16)
                w3[t, at, (r * legs + s) * LANES : (r * legs + s + 1) * LANES] = both

    steps = tiles * (quads // 2)

    def middle(n, _):
        second(n, n % 2)
        third(n - 1, (n + 1) % 2)
        return 0

    next_rows = down_rows(after[1:2])

    def build(c):
        for k in range(secs):
            delta = next_rows[k * half : (k + 1) * half, 0:chi] - after[0:1, 0:chi]
            for i in range(own):
                r, s = divmod(c * own + i, legs)
                gap = after[2:3, r : r + 1] - after[2:3, s : s + 1]
                value = jnp.where(delta == gap, right_all[k, c, i].astype(F32), 0.0)
                spread(value, rhs4[c], k * half, i)

    def last(c):
        seen = set()
        for t in range(tiles):
            part = lax.dot_general(
                w3[t, :, c * own * LANES : (c + 1) * own * LANES], rhs4[c][t],
                (((1,), (1,)), ((), ())), preferred_element_type=F32,
            )
            for k, (g, _, _) in enumerate(pieces[t]):
                value = part[:, k * LANES : (k + 1) * LANES]
                if c > 0 or g in seen:
                    value += image_s[g * block : (g + 1) * block]
                seen.add(g)
                image_s[g * block : (g + 1) * block] = value

    stops = [1] + [steps * p // 18 for p in (8, 12, 15)] + [steps]
    second(0, 0)
    lax.fori_loop(stops[0], stops[1], middle, 0, unroll=True)
    hear(1)
    tell(2)
    arrived(0)
    lax.fori_loop(stops[1], stops[2], middle, 0, unroll=True)
    hear(2)
    for n in range(3, rounds):
        tell(n)
        hear(n)
    passed(0)
    build(0)
    lax.fori_loop(stops[2], stops[3], middle, 0, unroll=True)
    arrived(1)
    lax.fori_loop(stops[3], stops[4], middle, 0, unroll=True)
    third(steps - 1, (steps - 1) % 2)
    for c in range(1, chunks):
        passed(c)
        if c + 1 < chunks:
            arrived(c + 1)
        last(c - 1)
        build(c)
    last(chunks - 1)

    diff[...] = fresh_rows + after[1:2]
    odd = diff[mine, 0:chi]
    odd = odd - 2.0 * jnp.floor(odd * 0.5)
    total_sq = jnp.zeros((half, chi), F32)
    for d in range(legs):
        for e in range(legs):
            value = image_s[pl.ds(d * legs + e, half, stride=pad), 0:chi]
            parity = ((vert_sm[1, d] + vert_sm[1, e]) & 1).astype(F32)
            value = jnp.where(odd == parity, value, 0.0)
            clean_s[d * legs + e] = value
            total_sq += value * value
    part = jnp.sum(jnp.sum(total_sq, axis=0, keepdims=True), axis=1, keepdims=True)
    stage[...] = jnp.broadcast_to(part, stage.shape)

    def close_copy(k, source):
        return pltpu.make_async_remote_copy(
            src_ref=stage, dst_ref=close_slots.at[source], send_sem=close_send.at[k], recv_sem=close_recv.at[source],
            device_id=partner(k), device_id_type=MESH,
        )

    def far_copy(k, d):
        return pltpu.make_async_remote_copy(
            src_ref=stage, dst_ref=slots.at[cols - 1 - k, me_sec], send_sem=far_send, recv_sem=far_recv,
            device_id=(column(k), d), device_id_type=MESH,
        )

    def far_all():
        return pltpu.make_async_remote_copy(
            src_ref=slots, dst_ref=slots, send_sem=far_send, recv_sem=far_recv,
            device_id=(before, me_sec), device_id_type=MESH,
        )

    def send(k, _):
        for d in range(secs):
            far_copy(k, d).start()
        return 0

    for k in range(1, secs):
        close_copy(k, me_sec).start()
    lax.fori_loop(1, cols, send, 0, unroll=cols <= 16)
    site = jnp.broadcast_to(part, stage.shape)
    for k in range(1, secs):
        source = lax.rem(me_sec + k, secs)
        close_copy(k, source).wait_recv()
        site = site + close_slots[source]
    scale = lax.rsqrt(site[0:1, 0:1] / count + 1e-06)
    for i in range(square):
        out_ref[i] = (clean_s[i] * scale).astype(BF16)
    charge_copy().wait_send()
    for k in range(1, secs):
        mps_copy(k, me_sec).wait_send()
        close_copy(k, me_sec).wait_send()
        for c in range(chunks):
            right_pass(c, k, me_sec).wait_send()
    for c in range(chunks):
        right_copy(c).wait_send()
    far_all().wait_recv()
    sums = jnp.sum(slots[...], axis=1) / count
    logs = jnp.sum(0.5 * jnp.log(sums + 1e-06), axis=0) + 0.5 * jnp.log(site / count + 1e-06)
    log_ref[...] = logs[0:1, 0:1] / cols
    far_all().wait_send()


def local(mps, ket, left_proj, right_proj, bond_charge, new_charge, link_charge, vert_charge):
    half, chi, legs = left_proj.shape[1:4]
    phys = ket.shape[5]
    assert phys == 2
    square = legs * legs
    cols, secs = lax.axis_size("col"), lax.axis_size("sec")
    group, tiles, quads, pad, pieces = layout(chi, half, legs)
    deep, block = legs * pad, quads * pad
    chunks = 3
    own = square // chunks
    assert deep <= 2 * LANES
    arrays = [
        left_proj[0].transpose(2, 3, 0, 1).reshape(square, half, chi),
        mps[0].transpose(1, 2, 0, 3).reshape(square, half, chi),
        right_proj[0].transpose(1, 2, 3, 0).reshape(square, half, chi),
        ket[0].transpose(0, 1, 2, 4, 3).reshape(square * legs * phys, legs),
        bond_charge,
        new_charge,
        link_charge,
        link_charge,
        vert_charge[0],
    ]
    far = pl.BlockSpec(memory_space=pl.ANY)
    near = pl.BlockSpec(memory_space=pltpu.VMEM)
    scalar = pl.BlockSpec(memory_space=pltpu.SMEM)
    image, logs = pl.pallas_call(
        functools.partial(chain, legs, phys, chi * square * chi, cols, secs),
        in_specs=[far] * 3 + [near] * 4 + [scalar] * 2,
        out_specs=[near, near],
        out_shape=[jax.ShapeDtypeStruct((square, half, chi), BF16), jax.ShapeDtypeStruct((1, 1), F32)],
        scratch_shapes=[
            pltpu.VMEM((square, half, chi), BF16),
            pltpu.VMEM((secs, square, half, chi), BF16),
            pltpu.VMEM((secs, chunks, own, half, chi), BF16),
            pltpu.VMEM((half * pad, LANES), F32),
            pltpu.VMEM((half * pad, LANES), BF16),
            pltpu.VMEM((tiles, 2 * LANES, square * LANES), BF16),
            [pltpu.VMEM((tiles, 2 * LANES, own * LANES), BF16) for _ in range(chunks)],
            pltpu.VMEM((phys, deep, 2 * LANES), F32),
            pltpu.VMEM((deep, 2 * LANES), F32),
            pltpu.VMEM((tiles, quads // 2, legs, deep, 2 * LANES), BF16),
            pltpu.VMEM((2, legs, deep, 2 * LANES), BF16),
            pltpu.VMEM((tiles, block, square * LANES), BF16),
            pltpu.VMEM((half * pad, LANES), F32),
            pltpu.VMEM((square, half, chi), F32),
            pltpu.VMEM((8, LANES), jnp.int32),
            pltpu.VMEM((8, LANES), jnp.int32),
            pltpu.VMEM((LANES, LANES), F32),
            pltpu.VMEM((legs, deep, LANES), BF16),
            pltpu.VMEM((tiles, quads // 2, 16, 2 * LANES), BF16),
            pltpu.VMEM((1, LANES), F32),
            pltpu.VMEM((cols - 1, secs, 1, LANES), F32),
            pltpu.VMEM((secs, 1, LANES), F32),
            pltpu.SemaphoreType.DMA((2,)),
            pltpu.SemaphoreType.DMA((secs,)),
            pltpu.SemaphoreType.DMA((1 + secs,)),
            pltpu.SemaphoreType.DMA((chunks,)),
            pltpu.SemaphoreType.DMA((chunks,)),
            pltpu.SemaphoreType.DMA((chunks, secs)),
            pltpu.SemaphoreType.DMA((chunks, secs)),
            pltpu.SemaphoreType.REGULAR((max(1, (cols // 2 - 1).bit_length()),)),
            pltpu.SemaphoreType.DMA,
            pltpu.SemaphoreType.DMA,
            pltpu.SemaphoreType.DMA((secs,)),
            pltpu.SemaphoreType.DMA((secs,)),
        ],
        compiler_params=pltpu.CompilerParams(
            vmem_limit_bytes=62 * 1024 * 1024,
            collective_id=0,
            has_side_effects=True,
        ),
    )(*arrays)
    new_mps = image.reshape(legs, legs, half, chi).transpose(2, 0, 1, 3)[None]
    return (new_mps, logs[0, 0])


def solution(mesh):
    placed = (
        P("col", "sec", None, None, None),
        P("col", None, None, None, None, None),
        P("col", "sec", None, None, None),
        P("col", None, None, None, "sec"),
        P("col", None),
        P("col", None),
        P("col", None),
        P("col", None, None),
    )
    return jax.shard_map(
        local,
        mesh=mesh,
        in_specs=placed,
        out_specs=(P("col", "sec", None, None, None), P()),
        check_vma=False,
    )
```

```python
import functools
import math

import jax
import jax.numpy as jnp
from jax import lax
from jax.experimental import pallas as pl
from jax.experimental.pallas import tpu as pltpu
from jax.sharding import PartitionSpec as P

LANES = 128
F32 = jnp.float32
BF16 = jnp.bfloat16
MESH = pl.DeviceIdType.MESH


def layout(chi, half, legs):
    span = math.lcm(chi, LANES)
    group, tiles = span // chi, span // LANES
    pieces = []
    for t in range(tiles):
        row = []
        for g in range(group):
            lo, hi = max(LANES * t, chi * g), min(LANES * (t + 1), chi * (g + 1))
            if lo < hi:
                row.append((g, lo - LANES * t, hi - LANES * t))
        pieces.append(row)
    assert all(len(row) == 2 and row[1][0] == row[0][0] + 1 for row in pieces)
    assert half % (2 * group) == 0 and half % 16 == 0 and chi <= LANES and legs % 2 == 0
    pad = -(-legs * legs // 8) * 8
    return group, tiles, half // group, pad, pieces


def chain(
    legs, phys, count, cols, secs,
    left_hbm, mps_hbm, right_hbm, ket_hbm, bond_hbm, fresh_hbm, link_hbm, link_far, vert_far,
    out_ref, log_ref,
    ket_ref, bond_ref, fresh_ref, link_ref, link_sm, vert_sm, right_v, left_v, mps_all, right_all, left_s, left_b, rhs1, rhs4, raw_s, whole_s, w1, w2, w3, image_s, clean_s,
    charge_here, charge_next, diff, rowkey, lanekey,
    stage, slots, close_slots, local_sem, near_send, near_recv, chunk_send, chunk_recv, pass_send, pass_recv,
    known, far_send, far_recv, close_send, close_recv,
):
    square = legs * legs
    half, chi = left_v.shape[1:]
    group, tiles, quads, pad, pieces = layout(chi, half, legs)
    deep = legs * pad
    block = quads * pad
    pairs = legs // 2
    me_col, me_sec = lax.axis_index("col"), lax.axis_index("sec")
    before = lax.rem(me_col + cols - 1, cols)
    barrier = pltpu.get_barrier_semaphore()
    mine = pl.ds(pl.multiple_of(me_sec * half, 16), half)

    chunks = right_all.shape[1]
    own = right_all.shape[2]

    def column(k):
        return lax.rem(me_col + k + cols, cols)

    def partner(k):
        return (me_col, lax.rem(me_sec + k, secs))

    def charge_copy():
        return pltpu.make_async_remote_copy(
            src_ref=charge_here, dst_ref=charge_next, send_sem=near_send.at[0], recv_sem=near_recv.at[0],
            device_id=(before, me_sec), device_id_type=MESH,
        )

    def mps_copy(k, source):
        return pltpu.make_async_remote_copy(
            src_ref=mps_all.at[source], dst_ref=mps_all.at[source], send_sem=near_send.at[k],
            recv_sem=near_recv.at[1 + source],
            device_id=partner(k), device_id_type=MESH,
        )

    def right_copy(c):
        return pltpu.make_async_remote_copy(
            src_ref=right_v.at[pl.ds(c * own, own)], dst_ref=right_all.at[me_sec, c],
            send_sem=chunk_send.at[c], recv_sem=chunk_recv.at[c],
            device_id=(before, me_sec), device_id_type=MESH,
        )

    def right_pass(c, k, source):
        return pltpu.make_async_remote_copy(
            src_ref=right_all.at[source, c], dst_ref=right_all.at[source, c],
            send_sem=pass_send.at[c, k], recv_sem=pass_recv.at[c, source],
            device_id=partner(k), device_id_type=MESH,
        )

    def arrived(c):
        right_copy(c).wait_recv()
        for k in range(1, secs):
            right_pass(c, k, me_sec).start()

    def passed(c):
        for k in range(1, secs):
            right_pass(c, k, lax.rem(me_sec + k, secs)).wait_recv()

    rounds = max(1, (cols // 2 - 1).bit_length())

    def tell(n):
        if n < rounds:
            for side in (-1, 1):
                pl.semaphore_signal(
                    known.at[n], inc=1, device_id=(column(side * 2**n), me_sec), device_id_type=MESH
                )

    def hear(n):
        if n < rounds:
            pl.semaphore_wait(known.at[n], 2)

    def down_rows(row):
        return jnp.broadcast_to(row, (LANES, LANES)).T

    def over(value, by):
        return jnp.floor((value + 0.5) * (1.0 / by))

    def axis(shape, dim):
        return lax.broadcasted_iota(jnp.int32, shape, dim).astype(F32)

    def chosen(index, values):
        return sum(jnp.where(index == float(i), v, 0.0) for i, v in enumerate(values))

    for k in range(1, secs):
        pl.semaphore_signal(barrier, inc=1, device_id=partner(k), device_id_type=MESH)
    for side in (-1, 1):
        pl.semaphore_signal(barrier, inc=1, device_id=(column(side), me_sec), device_id_type=MESH)
    load_left = pltpu.make_async_copy(left_hbm, left_v, local_sem.at[0])
    load_mps = pltpu.make_async_copy(mps_hbm, mps_all.at[me_sec], local_sem.at[1])
    small = [(bond_hbm, bond_ref), (fresh_hbm, fresh_ref), (link_hbm, link_ref), (link_far, link_sm), (vert_far, vert_sm)]
    small = [pltpu.make_async_copy(a, b, local_sem.at[3 + i]) for i, (a, b) in enumerate(small)]
    load_right = pltpu.make_async_copy(right_hbm, right_v, local_sem.at[8])
    load_ket = pltpu.make_async_copy(ket_hbm, ket_ref, local_sem.at[2])
    for copy in small + [load_left, load_mps, load_ket, load_right]:
        copy.start()
    left_s[...] = jnp.zeros_like(left_s)
    for t in range(tiles):
        for k in range(2):
            rhs1[t, k * LANES + chi : (k + 1) * LANES] = jnp.zeros((LANES - chi, square * LANES), BF16)
    for copy in small:
        copy.wait()
    charge_here[...] = jnp.zeros_like(charge_here)
    charge_here[0:1, 0:chi] = bond_ref[...]
    charge_here[1:2, 0:chi] = fresh_ref[...]
    charge_here[2:3, 0:legs] = link_ref[...]
    here = charge_here[...].astype(F32)
    diff[...] = down_rows(here[1:2]) - here[0:1]
    gaps_here = diff[mine, 0:chi]
    fresh_rows = down_rows(here[1:2])
    lane = lax.broadcasted_iota(jnp.int32, (1, LANES), 1)

    def inside(lo, hi):
        return jnp.logical_and(lane >= lo, lane < hi)

    def turned(value):
        rest = jnp.zeros(value.shape[:-1] + (LANES - chi,), value.dtype)
        wide = jnp.concatenate([value, rest], axis=1)
        return [wide if (chi * g) % LANES == 0 else pltpu.roll(wide, (chi * g) % LANES, 1) for g in range(group)]

    def spread(value, dest, at, place):
        rolled = turned(value)
        for t in range(tiles):
            for k, (g, lo, hi) in enumerate(pieces[t]):
                piece = jnp.where(inside(lo, hi), rolled[g], 0.0)
                dest[t, pl.ds(k * LANES + at, half), place * LANES : (place + 1) * LANES] = piece.astype(BF16)

    load_left.wait()
    for l in range(legs):
        for m in range(legs):
            gap = (link_sm[0, l] - link_sm[0, m]).astype(F32)
            value = jnp.where(gaps_here == gap, left_v[l * legs + m].astype(F32), 0.0)
            left_s[pl.ds(l * legs + m, half, stride=pad), 0:chi] = value
    left_b[...] = left_s[...].astype(BF16)

    def half_one(source):
        at = pl.multiple_of(source * half, 16)
        for u in range(legs):
            for v in range(legs):
                spread(mps_all[source, u * legs + v].astype(F32), rhs1, at, v * legs + u)

    load_mps.wait()
    half_one(me_sec)

    small = (pad, 2 * LANES)
    row_in = axis(small, 0)
    row_mid = over(row_in, legs)
    row_last = row_in - legs * row_mid
    col = axis(small, 1)
    col_top = over(col, pad)
    col_in = col - pad * col_top
    col_mid = over(col_in, legs)
    col_last = col_in - legs * col_mid
    keys = square * legs * phys
    line = axis((pad, keys), 1)
    line_p = over(line, phys)
    line_d = line_p - legs * over(line_p, legs)
    line_p = line - phys * line_p
    tall = (keys, 2 * LANES)
    tall_in = over(axis(tall, 0), legs * phys)
    tall_u = over(tall_in, legs)
    tall_l = tall_in - legs * tall_u
    tall_col = axis(tall, 1)
    tall_top = over(tall_col, pad)
    tall_mid = over(tall_col - pad * tall_top, legs)
    spread_c = jnp.where(jnp.logical_and(tall_u == tall_top, tall_l == tall_mid), 1.0, 0.0).astype(BF16)
    load_ket.wait()
    lead = jnp.where(over(axis((deep, legs), 0), pad) == axis((deep, legs), 1), 1.0, 0.0).astype(BF16)
    grown = lax.dot_general(lead, ket_ref[...], (((1,), (1,)), ((), ())), preferred_element_type=F32)
    same_d = line_d == row_last[:, 0:1]
    for p in range(phys):
        keep = jnp.logical_and(same_d, line_p == float(p))
        picked = [jnp.where(keep, grown[r * pad : (r + 1) * pad], 0.0) for r in range(legs)]
        picked = jnp.concatenate(picked, axis=0).astype(BF16)
        raw_s[p] = jnp.dot(picked, spread_c, preferred_element_type=F32)

    load_right.wait()
    pl.semaphore_wait(barrier, secs + 1)
    charge_copy().start()
    for k in range(1, secs):
        mps_copy(k, me_sec).start()
    for c in range(chunks):
        right_copy(c).start()
    tell(0)

    for k in range(1, secs):
        source = lax.rem(me_sec + k, secs)
        mps_copy(k, source).wait_recv()
        half_one(source)

    for t in range(tiles):
        lhs = jnp.concatenate([left_b[g * block : (g + 1) * block] for g, _, _ in pieces[t]], axis=1)

        def first(i, _, t=t, lhs=lhs):
            part = jnp.dot(lhs, rhs1[t, :, pl.ds(pl.multiple_of(i * 2 * LANES, 2 * LANES), 2 * LANES)], preferred_element_type=F32)
            for q in range(quads):
                rows = part[q * pad : (q + 1) * pad]
                both = jnp.concatenate([rows[:, :LANES], rows[:, LANES:]], axis=0).astype(BF16)
                at = pl.ds(pl.multiple_of((i % pairs) * 2 * pad, 16), 2 * pad)
                w1[t, q // 2, i // pairs, at, (q % 2) * LANES : (q % 2 + 1) * LANES] = both
            return 0

        lax.fori_loop(0, pairs * legs, first, 0, unroll=True)

    hear(0)
    tell(1)
    charge_copy().wait_recv()
    after = charge_next[...].astype(F32)

    col_key = chosen(col_top, [vert_sm[0, i].astype(F32) for i in range(legs)])
    col_key += chosen(col_mid, [link_sm[0, i].astype(F32) for i in range(legs)])
    row_key = chosen(row_last, [vert_sm[1, i].astype(F32) for i in range(legs)])
    same = jnp.logical_and(row_mid == col_last, jnp.logical_and(row_in < square, col_in < square))
    for r in range(legs):
        lack = col_key - row_key - after[2:3, r : r + 1]
        value = jnp.zeros(small, F32)
        for p in range(phys):
            value += jnp.where(lack == float(p), raw_s[p, r * pad : (r + 1) * pad, :], 0.0)
        whole_s[r * pad : (r + 1) * pad, :] = jnp.where(same, value, 0.0)
    both_rows = whole_s[:, 0:deep].astype(BF16)

    ups = [vert_sm[0, i].astype(F32) for i in range(legs)]
    mid_key = chosen(row_last, [link_sm[0, i].astype(F32) for i in range(legs)])
    mid_key -= chosen(row_mid, [link_sm[0, i].astype(F32) for i in range(legs)])
    for v in range(legs):
        for u in range(pairs):
            pair = jnp.concatenate([mid_key[:, :LANES] + (ups[2 * u + k] - ups[v]) for k in range(2)], axis=0)
            rowkey[v, u * 2 * pad : (u + 1) * 2 * pad] = pair.astype(BF16)
    turned_next = turned(after[0:1, 0:chi])
    diff[...] = fresh_rows
    for t in range(tiles):
        for q in range(quads):
            key = jnp.zeros((16, LANES), F32)
            for g, lo, hi in pieces[t]:
                fresh = diff[pl.ds(me_sec * half + g * quads + q, 1), :]
                key += jnp.where(inside(lo, hi), turned_next[g] - fresh, 0.0)
            lanekey[t, q // 2, :, (q % 2) * LANES : (q % 2 + 1) * LANES] = key.astype(BF16)

    def second(n, slot):
        t, j = n // (quads // 2), n % (quads // 2)
        key = lanekey[t, j][None]
        for vp in range(pairs):
            parts = []
            for k in range(2):
                rows = rowkey[2 * vp + k]
                rows = jnp.concatenate([rows, rows], axis=1).reshape(deep // 16, 16, 2 * LANES)
                value = w1[t, j, 2 * vp + k].reshape(deep // 16, 16, 2 * LANES)
                value = jnp.where(rows == key, value, jnp.zeros_like(value)).reshape(deep, 2 * LANES)
                parts.append(jnp.dot(both_rows, value, preferred_element_type=F32))
            for r in range(legs):
                both = jnp.concatenate([part[r * pad : (r + 1) * pad] for part in parts], axis=0)
                w2[slot, r, vp * 2 * pad : (vp + 1) * 2 * pad, :] = both.astype(BF16)

    def third(n, slot):
        t, j = n // (quads // 2), n % (quads // 2)
        at = pl.ds(pl.multiple_of(j * 2 * pad, 16), 2 * pad)
        for r in range(legs):
            part = jnp.dot(both_rows, w2[slot, r], preferred_element_type=F32)
            for s in range(legs):
                rows = part[s * pad : (s + 1) * pad]
                both = jnp.concatenate([rows[:, :LANES], rows[:, LANES:]], axis=0).astype(BF16)
                w3[t, at, (r * legs + s) * LANES : (r * legs + s + 1) * LANES] = both

    steps = tiles * (quads // 2)

    def middle(n, _):
        second(n, n % 2)
        third(n - 1, (n + 1) % 2)
        return 0

    next_rows = down_rows(after[1:2])

    def build(c, k, i):
        delta = next_rows[k * half : (k + 1) * half, 0:chi] - after[0:1, 0:chi]
        r, s = divmod(c * own + i, legs)
        gap = after[2:3, r : r + 1] - after[2:3, s : s + 1]
        value = jnp.where(delta == gap, right_all[k, c, i].astype(F32), 0.0)
        spread(value, rhs4[c], k * half, i)

    def share(c, n, of):
        for at in range(secs * own * n // of, secs * own * (n + 1) // of):
            build(c, at // own, at % own)

    def last(c, t):
        part = lax.dot_general(
            w3[t, :, c * own * LANES : (c + 1) * own * LANES], rhs4[c][t],
            (((1,), (1,)), ((), ())), preferred_element_type=F32,
        )
        for k, (g, _, _) in enumerate(pieces[t]):
            value = part[:, k * LANES : (k + 1) * LANES]
            if c > 0 or k == 0 and t > 0:
                value += image_s[g * block : (g + 1) * block]
            image_s[g * block : (g + 1) * block] = value

    stops = [1] + [steps * p // 18 for p in (8, 12, 15)] + [steps]
    second(0, 0)
    lax.fori_loop(stops[0], stops[1], middle, 0, unroll=True)
    hear(1)
    tell(2)
    arrived(0)
    lax.fori_loop(stops[1], stops[2], middle, 0, unroll=True)
    hear(2)
    for n in range(3, rounds):
        tell(n)
        hear(n)
    passed(0)
    of = 2 * (steps - stops[2])
    for n in range(stops[2], steps):
        if n == stops[3]:
            arrived(1)
        second(n, n % 2)
        share(0, 2 * (n - stops[2]), of)
        third(n - 1, (n + 1) % 2)
        share(0, 2 * (n - stops[2]) + 1, of)
    third(steps - 1, (steps - 1) % 2)
    for c in range(1, chunks):
        passed(c)
        if c + 1 < chunks:
            arrived(c + 1)
        for t in range(tiles):
            share(c, t, tiles)
            last(c - 1, t)
    for t in range(tiles):
        last(chunks - 1, t)

    diff[...] = fresh_rows + after[1:2]
    odd = diff[mine, 0:chi]
    odd = odd - 2.0 * jnp.floor(odd * 0.5)
    total_sq = jnp.zeros((half, chi), F32)
    for d in range(legs):
        for e in range(legs):
            value = image_s[pl.ds(d * legs + e, half, stride=pad), 0:chi]
            parity = ((vert_sm[1, d] + vert_sm[1, e]) & 1).astype(F32)
            value = jnp.where(odd == parity, value, 0.0)
            clean_s[d * legs + e] = value
            total_sq += value * value
    part = jnp.sum(jnp.sum(total_sq, axis=0, keepdims=True), axis=1, keepdims=True)
    stage[...] = jnp.broadcast_to(part, stage.shape)

    def close_copy(k, source):
        return pltpu.make_async_remote_copy(
            src_ref=stage, dst_ref=close_slots.at[source], send_sem=close_send.at[k], recv_sem=close_recv.at[source],
            device_id=partner(k), device_id_type=MESH,
        )

    def far_copy(k, d):
        return pltpu.make_async_remote_copy(
            src_ref=stage, dst_ref=slots.at[cols - 1 - k, me_sec], send_sem=far_send, recv_sem=far_recv,
            device_id=(column(k), d), device_id_type=MESH,
        )

    def far_all():
        return pltpu.make_async_remote_copy(
            src_ref=slots, dst_ref=slots, send_sem=far_send, recv_sem=far_recv,
            device_id=(before, me_sec), device_id_type=MESH,
        )

    def send(k, _):
        for d in range(secs):
            far_copy(k, d).start()
        return 0

    for k in range(1, secs):
        close_copy(k, me_sec).start()
    lax.fori_loop(1, cols, send, 0, unroll=cols <= 16)
    site = jnp.broadcast_to(part, stage.shape)
    for k in range(1, secs):
        source = lax.rem(me_sec + k, secs)
        close_copy(k, source).wait_recv()
        site = site + close_slots[source]
    scale = lax.rsqrt(site[0:1, 0:1] / count + 1e-06)
    for i in range(square):
        out_ref[i] = (clean_s[i] * scale).astype(BF16)
    charge_copy().wait_send()
    for k in range(1, secs):
        mps_copy(k, me_sec).wait_send()
        close_copy(k, me_sec).wait_send()
        for c in range(chunks):
            right_pass(c, k, me_sec).wait_send()
    for c in range(chunks):
        right_copy(c).wait_send()
    far_all().wait_recv()
    sums = jnp.sum(slots[...], axis=1) / count
    logs = jnp.sum(0.5 * jnp.log(sums + 1e-06), axis=0) + 0.5 * jnp.log(site / count + 1e-06)
    log_ref[...] = logs[0:1, 0:1] / cols
    far_all().wait_send()


def local(mps, ket, left_proj, right_proj, bond_charge, new_charge, link_charge, vert_charge):
    half, chi, legs = left_proj.shape[1:4]
    phys = ket.shape[5]
    assert phys == 2
    square = legs * legs
    cols, secs = lax.axis_size("col"), lax.axis_size("sec")
    group, tiles, quads, pad, pieces = layout(chi, half, legs)
    deep, block = legs * pad, quads * pad
    chunks = 3
    own = square // chunks
    assert deep <= 2 * LANES
    arrays = [
        left_proj[0].transpose(2, 3, 0, 1).reshape(square, half, chi),
        mps[0].transpose(1, 2, 0, 3).reshape(square, half, chi),
        right_proj[0].transpose(1, 2, 3, 0).reshape(square, half, chi),
        ket[0].transpose(0, 1, 2, 4, 3).reshape(square * legs * phys, legs),
        bond_charge,
        new_charge,
        link_charge,
        link_charge,
        vert_charge[0],
    ]
    far = pl.BlockSpec(memory_space=pl.ANY)
    near = pl.BlockSpec(memory_space=pltpu.VMEM)
    image, logs = pl.pallas_call(
        functools.partial(chain, legs, phys, chi * square * chi, cols, secs),
        in_specs=[far] * len(arrays),
        out_specs=[near, near],
        out_shape=[pltpu.VMEM((square, half, chi), BF16), jax.ShapeDtypeStruct((1, 1), F32)],
        scratch_shapes=[
            pltpu.VMEM(arrays[3].shape, BF16),
            pltpu.VMEM((1, chi), jnp.int32),
            pltpu.VMEM((1, chi), jnp.int32),
            pltpu.VMEM((1, legs), jnp.int32),
            pltpu.SMEM((1, legs), jnp.int32),
            pltpu.SMEM((2, legs), jnp.int32),
            pltpu.VMEM((square, half, chi), BF16),
            pltpu.VMEM((square, half, chi), BF16),
            pltpu.VMEM((secs, square, half, chi), BF16),
            pltpu.VMEM((secs, chunks, own, half, chi), BF16),
            pltpu.VMEM((half * pad, LANES), F32),
            pltpu.VMEM((half * pad, LANES), BF16),
            pltpu.VMEM((tiles, 2 * LANES, square * LANES), BF16),
            [pltpu.VMEM((tiles, 2 * LANES, own * LANES), BF16) for _ in range(chunks)],
            pltpu.VMEM((phys, deep, 2 * LANES), F32),
            pltpu.VMEM((deep, 2 * LANES), F32),
            pltpu.VMEM((tiles, quads // 2, legs, deep, 2 * LANES), BF16),
            pltpu.VMEM((2, legs, deep, 2 * LANES), BF16),
            pltpu.VMEM((tiles, block, square * LANES), BF16),
            pltpu.VMEM((half * pad, LANES), F32),
            pltpu.VMEM((square, half, chi), F32),
            pltpu.VMEM((8, LANES), jnp.int32),
            pltpu.VMEM((8, LANES), jnp.int32),
            pltpu.VMEM((LANES, LANES), F32),
            pltpu.VMEM((legs, deep, LANES), BF16),
            pltpu.VMEM((tiles, quads // 2, 16, 2 * LANES), BF16),
            pltpu.VMEM((1, LANES), F32),
            pltpu.VMEM((cols - 1, secs, 1, LANES), F32),
            pltpu.VMEM((secs, 1, LANES), F32),
            pltpu.SemaphoreType.DMA((9,)),
            pltpu.SemaphoreType.DMA((secs,)),
            pltpu.SemaphoreType.DMA((1 + secs,)),
            pltpu.SemaphoreType.DMA((chunks,)),
            pltpu.SemaphoreType.DMA((chunks,)),
            pltpu.SemaphoreType.DMA((chunks, secs)),
            pltpu.SemaphoreType.DMA((chunks, secs)),
            pltpu.SemaphoreType.REGULAR((max(1, (cols // 2 - 1).bit_length()),)),
            pltpu.SemaphoreType.DMA,
            pltpu.SemaphoreType.DMA,
            pltpu.SemaphoreType.DMA((secs,)),
            pltpu.SemaphoreType.DMA((secs,)),
        ],
        compiler_params=pltpu.CompilerParams(
            vmem_limit_bytes=60 * 1024 * 1024,
            collective_id=0,
            has_side_effects=True,
        ),
    )(*arrays)
    new_mps = image.reshape(legs, legs, half, chi).transpose(2, 0, 1, 3)[None]
    return (new_mps, logs[0, 0])


def solution(mesh):
    placed = (
        P("col", "sec", None, None, None),
        P("col", None, None, None, None, None),
        P("col", "sec", None, None, None),
        P("col", None, None, None, "sec"),
        P("col", None),
        P("col", None),
        P("col", None),
        P("col", None, None),
    )
    return jax.shard_map(
        local,
        mesh=mesh,
        in_specs=placed,
        out_specs=(P("col", "sec", None, None, None), P()),
        check_vma=False,
    )
```
